32 devices in a mesh: tile: 8 (over z, x), pos: 4 (over y, core).
Axes of the slice: x: 2, y: 2, z: 4, core: 2. Of those that a mesh axis runs over, the one named last changes fastest.
Arguments:
- object_tiles: bfloat16 [8, 2, 512, 512], P('tile', None, 'pos'), may hold values from -4.1875 to 4.1875
- probe: float32 [2, 256, 256], replicated, may hold values from -4.2 to 4.2
- frames: bfloat16 [512, 256, 256], P(('tile', 'pos')), may hold values from 0 to 60, as said below
- offsets: int32 [2, 512], P(None, ('tile', 'pos')), may hold values from 1 to 511
Outputs:
- shifts: float32 [2, 512], P(None, ('tile', 'pos'))
- losses: float32 [512], P(('tile', 'pos'))
The draws below stay inside these ranges and needn't reach their ends.
Inputs may be any that keep to these rules, and one draw needn't show every extreme that they name: `frames`: amplitudes are not negative.
All inputs are finite; a program needn't handle non-finite values.
Results may differ from the reference program's by a relative error of at most 0.0097.
Values may be sent and summed in bfloat16 or wider, within the bound.
A program may use at most 128 MiB of HBM per device.

```python
import math
import jax
import jax.numpy as jnp
from jax import lax

PROBE = 256
GC = 4
POS_DEV = 16
CORE = 512
TILES = 8
POSITIONS = 512
N_TILE = 8
N_POS = 4


def draw_frames(key, part):
    ramp_scale = 1.0 + 2.0 * jnp.arange(POSITIONS, dtype=jnp.float32) / (POSITIONS - 1)
    normal_base = jax.random.normal(jax.random.fold_in(key, 5), (POSITIONS, PROBE, PROBE), jnp.float32)
    amplitude = jnp.minimum(jnp.abs(normal_base), 5.0) * ramp_scale[:, None, None]
    return amplitude.astype(jnp.bfloat16)


def with_ends(values, key, low, high):
    extent = values.shape
    index_at = [jax.random.randint(jax.random.fold_in(key, axis), (), 0, extent[axis]) for axis in range(len(extent))]
    values = values.at[tuple(index_at)].set(low)
    longest = extent.index(max(extent))
    index_at[longest] = (index_at[longest] + 1) % extent[longest]
    return values.at[tuple(index_at)].set(high)


def levels(stream_key, extent, split, least, high):
    loudness, own = 1.0, jax.random.fold_in(stream_key, 6)
    for dim, blocks in split:
        heights = jnp.exp(jax.random.uniform(jax.random.fold_in(own, dim), (blocks,), jnp.float32, least / len(split), high / len(split)))
        loudness = loudness * jnp.repeat(heights, extent[dim] // blocks).reshape([-1 if axis == dim else 1 for axis in range(len(extent))])
    return loudness


def centred(stream_key, dims, deviation, limit, split=(), kind=jnp.bfloat16):
    result = deviation * jax.random.normal(stream_key, dims, jnp.float32)
    if split:
        result = result * levels(stream_key, dims, split, -0.22, 0.18)
    return jnp.clip(result, -limit, limit).astype(kind)


def setup_inputs(seed: int = 0) -> dict:
    key_of = jax.random.split(jax.random.key(seed), 5)
    object_tiles = centred(key_of[0], (TILES, 2, CORE, CORE), 0.7, 4.1875, ((0, 8), (2, 4)))
    probe = centred(key_of[1], (2, PROBE, PROBE), 0.7, 4.2, (), jnp.float32)
    frames = draw_frames(jax.random.fold_in(key_of[4], 71), 0)
    offsets = with_ends(jax.random.randint(key_of[3], (2, POSITIONS), 1, CORE), jax.random.fold_in(key_of[3], 1), 1, CORE - 1).astype(jnp.int32)
    return dict(object_tiles=object_tiles, probe=probe, frames=frames, offsets=offsets)


def dft_tables(length_n):
    indices = jnp.arange(length_n, dtype=jnp.int32)
    products_mod = indices[:, None] * indices[None, :] % length_n
    angles = products_mod.astype(jnp.float32) * (2.0 * math.pi / length_n)
    factor = 1.0 / math.sqrt(length_n)
    return ((jnp.cos(angles) * factor).astype(jnp.bfloat16), (jnp.sin(angles) * factor).astype(jnp.bfloat16))

def matmul(left_m, right_m):
    return jnp.dot(left_m, right_m, preferred_element_type=jnp.float32)

def refine_ref(window, probe, detector, cosine_table, sine_table):
    window_f = window.astype(jnp.float32)
    patch = window_f[:, 1:-1, 1:-1]
    along_row = 0.5 * (window_f[:, 2:, 1:-1] - window_f[:, :-2, 1:-1])
    along_col = 0.5 * (window_f[:, 1:-1, 2:] - window_f[:, 1:-1, :-2])
    exit_re = (probe[0] * patch[0] - probe[1] * patch[1]).astype(jnp.bfloat16)
    exit_im = (probe[0] * patch[1] + probe[1] * patch[0]).astype(jnp.bfloat16)
    half_re = (matmul(cosine_table, exit_re) + matmul(sine_table, exit_im)).astype(jnp.bfloat16)
    half_im = (matmul(cosine_table, exit_im) - matmul(sine_table, exit_re)).astype(jnp.bfloat16)
    far_re = matmul(half_re, cosine_table) + matmul(half_im, sine_table)
    far_im = matmul(half_im, cosine_table) - matmul(half_re, sine_table)
    magnitude = jnp.sqrt(far_re * far_re + far_im * far_im)
    keep_part = 1.0 - detector.astype(jnp.float32) / jnp.maximum(magnitude, 0.25)
    resid_re = far_re * keep_part
    resid_im = far_im * keep_part
    loss_one = jnp.mean(resid_re * resid_re + resid_im * resid_im)
    round_re = resid_re.astype(jnp.bfloat16)
    round_im = resid_im.astype(jnp.bfloat16)
    inner_re = (matmul(cosine_table, round_re) - matmul(sine_table, round_im)).astype(jnp.bfloat16)
    inner_im = (matmul(cosine_table, round_im) + matmul(sine_table, round_re)).astype(jnp.bfloat16)
    wave_re = matmul(inner_re, cosine_table) - matmul(inner_im, sine_table)
    wave_im = matmul(inner_im, cosine_table) + matmul(inner_re, sine_table)

    def slope_of(derived):
        probed_re = probe[0] * derived[0] - probe[1] * derived[1]
        probed_im = probe[0] * derived[1] + probe[1] * derived[0]
        return jnp.sum(wave_re * probed_re + wave_im * probed_im)
    return (jnp.stack([slope_of(along_row), slope_of(along_col)]), loss_one)

def reference(object_tiles, probe, frames, offsets):
    region_rows = N_TILE // GC
    region_grid = object_tiles.reshape(region_rows, GC, 2, CORE, CORE)
    full_object = region_grid.transpose(2, 0, 3, 1, 4).reshape(2, region_rows * CORE, GC * CORE)
    margin = PROBE // 2
    padded = jnp.pad(full_object, ((0, 0), (margin, margin), (margin, margin)))
    indices = jnp.arange(POSITIONS, dtype=jnp.int32)
    region_of = indices // (POS_DEV * N_POS)
    starts_row = region_of // GC * CORE + offsets[0] - 1
    starts_col = region_of % GC * CORE + offsets[1] - 1
    cosine_table, sine_table = dft_tables(PROBE)

    def refine_at(position):
        detector, start_row, start_col = position
        window = lax.dynamic_slice(padded, (jnp.zeros((), jnp.int32), start_row.astype(jnp.int32), start_col.astype(jnp.int32)), (2, PROBE + 2, PROBE + 2))
        return refine_ref(window, probe, detector, cosine_table, sine_table)
    slopes, losses = lax.map(refine_at, (frames, starts_row, starts_col))
    total_sq = jnp.sum(slopes * slopes)
    norm_scale = jnp.sqrt(total_sq / POSITIONS + 1e-06)
    return ((-slopes / norm_scale).T, losses)
```

```python
import functools
import math

import jax
import jax.numpy as jnp
import numpy as np
from jax import lax
from jax.experimental import pallas as pl
from jax.experimental.pallas import tpu as pltpu
from jax.sharding import PartitionSpec as P

GC = 4
SENDS = 46
RECEIVES = 35
BATCH = 4
MESH_ID = pl.DeviceIdType.MESH


def dft_tables(length_n):
    indices = np.arange(length_n)
    products_mod = indices[:, None] * indices[None, :] % length_n
    angles = products_mod.astype(np.float32) * np.float32(2.0 * math.pi / length_n)
    factor = np.float32(1.0 / math.sqrt(length_n))
    cosine, sine = np.cos(angles) * factor, np.sin(angles) * factor
    forward = np.block([[cosine, sine], [-sine, cosine]])
    return jnp.asarray(forward, jnp.bfloat16), jnp.asarray(forward.T, jnp.bfloat16)


def gather_halo(n_tile, n_pos, margin, x_hbm, pad_ref, send_sems, recv_sems, local_sem, convert):
    t, p = lax.axis_index("tile"), lax.axis_index("pos")
    _, quarter, width = x_hbm.shape
    rows = pad_ref.shape[1] - 2 * margin
    last = rows // quarter - 1
    c, r = t % GC, t // GC
    core, half = p % 2, p // 2
    near, far = p + 1 - 2 * core, p + 2 - 4 * half
    near_far = near + 2 - 4 * half
    west, east = c > 0, c < GC - 1
    north, south = r > 0, r < n_tile // GC - 1
    yes = p >= 0
    both = jnp.logical_and
    tall, wide = rows + 2 * margin, width + 2 * margin

    barrier = pltpu.get_barrier_semaphore()
    me, count = t * n_pos + p, n_tile * n_pos
    for k in range(1, count):
        other = lax.rem(me + k, count)
        pl.semaphore_signal(barrier, inc=1, device_id=(other // n_pos, other % n_pos), device_id_type=MESH_ID)

    def block(q):
        return pl.ds(pl.multiple_of(margin + q * quarter, quarter), quarter)

    mine, its, nears, nears_far = block(p), block(far), block(near), block(near_far)
    above, below = slice(0, margin), slice(margin + rows, tall)
    top, bottom = slice(margin, 2 * margin), slice(rows, margin + rows)
    mid = slice(margin, margin + width)
    left, right = slice(0, margin), slice(margin + width, wide)
    first_cols, last_cols = slice(margin, 2 * margin), slice(width, margin + width)
    inner_cols = slice(2 * margin, width)
    strips = (first_cols, last_cols, inner_cols)
    sent = []

    def at(rows_at, cols_at):
        return pad_ref.at[:, rows_at, cols_at]

    own = pltpu.make_async_copy(x_hbm, at(mine, mid), local_sem)
    own.start()

    def zero(cond, rows_at, cols_at):
        @pl.when(cond)
        def _():
            part = at(rows_at, cols_at)
            part[...] = jnp.zeros(part.shape, part.dtype)

    zero(jnp.logical_not(west), slice(0, tall), left)
    zero(jnp.logical_not(east), slice(0, tall), right)
    zero(jnp.logical_not(north), above, slice(0, wide))
    zero(jnp.logical_not(south), below, slice(0, wide))

    def copy(index, src, dst, to_t, to_p, send_index):
        return pltpu.make_async_remote_copy(
            src_ref=src,
            dst_ref=dst,
            send_sem=send_sems.at[send_index],
            recv_sem=recv_sems.at[index],
            device_id=(to_t, to_p),
            device_id_type=MESH_ID,
        )

    def send(cond, index, src, dst, to_t, to_p):
        made = copy(index, src, dst, to_t, to_p, len(sent))
        sent.append((cond, made))

        @pl.when(cond)
        def _():
            made.start()

    def receive(cond, index, dst):
        @pl.when(cond)
        def _():
            copy(index, dst, dst, t, near, 0).wait_recv()

    own.wait()
    pl.semaphore_wait(barrier, count - 1)

    up, down = both(p == 0, north), both(p == last, south)
    native = jnp.logical_or(up, down)
    plain = jnp.logical_not(native)
    send(east, 0, at(mine, last_cols), at(mine, left), t + 1, p)
    send(west, 1, at(mine, first_cols), at(mine, right), t - 1, p)
    vertical = ((up, top, below, t - GC, 6), (down, bottom, above, t + GC, 9))
    for cond, src, dst, to_t, base in vertical:
        for k in range(2):
            send(cond, base + k, at(src, strips[k]), at(dst, strips[k]), to_t, far)
            send(cond, base + k, at(src, strips[k]), at(dst, strips[k]), to_t, p)
    for k in range(2):
        send(yes, 2 + k, at(mine, strips[k]), at(mine, strips[k]), t, far)
    for cond, src, dst, to_t, base in vertical:
        send(cond, base + 2, at(src, strips[2]), at(dst, strips[2]), to_t, far)
        send(cond, base + 2, at(src, strips[2]), at(dst, strips[2]), to_t, p)
    send(native, 4, at(mine, inner_cols), at(mine, inner_cols), t, far)
    send(yes, 5, at(mine, mid), at(mine, mid), t, near)

    receive(west, 0, at(mine, left))
    receive(east, 1, at(mine, right))
    send(west, 15, at(mine, left), at(mine, left), t, near)
    send(east, 16, at(mine, right), at(mine, right), t, near)
    receive(yes, 2, at(its, first_cols))
    send(west, 13, at(its, first_cols), at(its, right), t - 1, p)
    receive(yes, 3, at(its, last_cols))
    send(east, 12, at(its, last_cols), at(its, left), t + 1, p)
    send(plain, 4, at(mine, inner_cols), at(mine, inner_cols), t, far)
    send(yes, 14, at(its, first_cols), at(its, first_cols), t, near)
    send(yes, 33, at(its, last_cols), at(its, last_cols), t, near)
    convert(margin + p * quarter, quarter)

    halos = ((both(south, core == 0), below, 6, 19, 25), (both(north, core == 1), above, 9, 22, 27))
    for cond, area, base, shared, corner in halos:
        receive(cond, base, at(area, first_cols))
        send(both(cond, west), corner, at(area, first_cols), at(area, right), t - 1, p)
        receive(cond, base + 1, at(area, last_cols))
        send(both(cond, east), corner + 1, at(area, last_cols), at(area, left), t + 1, p)
        send(cond, shared, at(area, first_cols), at(area, first_cols), t, near)
        send(cond, shared + 1, at(area, last_cols), at(area, last_cols), t, near)

    receive(yes, 5, at(nears, mid))
    receive(west, 15, at(nears, left))
    receive(east, 16, at(nears, right))
    convert(margin + near * quarter, quarter)

    for cond, area, base, shared, corner in halos:
        receive(cond, base + 2, at(area, inner_cols))
        send(cond, shared + 2, at(area, inner_cols), at(area, inner_cols), t, near)
    receive(east, 13, at(its, right))
    send(east, 18, at(its, right), at(its, right), t, near)
    receive(west, 12, at(its, left))
    send(west, 17, at(its, left), at(its, left), t, near)
    for cond, area, base, shared, corner in halos:
        receive(both(cond, east), corner, at(area, right))
        send(both(cond, east), corner + 4, at(area, right), at(area, right), t, near)
        receive(both(cond, west), corner + 1, at(area, left))
        send(both(cond, west), corner + 5, at(area, left), at(area, left), t, near)
    receive(yes, 4, at(its, inner_cols))
    send(yes, 34, at(its, inner_cols), at(its, inner_cols), t, near)
    convert(margin + far * quarter, quarter)

    others = ((both(south, core == 1), below, 19, 25), (both(north, core == 0), above, 22, 27))
    for cond, area, shared, corner in others:
        for k in range(3):
            receive(cond, shared + k, at(area, strips[k]))
        receive(both(cond, east), corner + 4, at(area, right))
        receive(both(cond, west), corner + 5, at(area, left))
    convert(0, margin)
    convert(margin + rows, margin)
    receive(yes, 14, at(nears_far, first_cols))
    receive(yes, 33, at(nears_far, last_cols))
    receive(west, 17, at(nears_far, left))
    receive(east, 18, at(nears_far, right))
    receive(yes, 34, at(nears_far, inner_cols))
    convert(margin + near_far * quarter, quarter)
    for cond, made in sent:
        @pl.when(cond)
        def _():
            made.wait_send()


def shared_sum(n_tile, n_pos, mine_ref, others, send_sems, recv_sems):
    me = lax.axis_index("tile") * n_pos + lax.axis_index("pos")
    count = n_tile * n_pos
    copies = []
    for k in range(1, count):
        other = lax.rem(me + k, count)
        made = pltpu.make_async_remote_copy(
            src_ref=mine_ref,
            dst_ref=others.at[k - 1],
            send_sem=send_sems.at[k - 1],
            recv_sem=recv_sems.at[k - 1],
            device_id=(other // n_pos, other % n_pos),
            device_id_type=MESH_ID,
        )
        made.start()
        copies.append(made)
    for made in copies:
        made.wait()
    return jnp.sum(others[...], axis=0) + mine_ref[...]


def fold(value):
    return jnp.sum(value.reshape(-1, 8, value.shape[-1]), axis=0)


def refine_kernel(
    batch, steps, n_tile, n_pos, off_ref, x_hbm, probe_hbm, frames_hbm, fwd_hbm, bwd_hbm, out_ref,
    pad_ref, probe_ref, fwd_ref, bwd_ref, frames_ref, planes, patch, slant, exits, halves, resid, inner, sums,
    send_sems, recv_sems, local_sems, line_ref, others, sum_sends, sum_recvs,
):
    n = probe_ref.shape[1]
    tall, wide = pad_ref.shape[1], pad_ref.shape[2]
    lanes = 128
    blocks = n // lanes

    def convert(first, height):
        @pl.loop(0, height // 32)
        def _(i):
            at = pl.ds(pl.multiple_of(first + i * 32, 32), 32)
            lower = pl.ds(pl.multiple_of(first + i * 32 + 8, 8), 32)
            for part in range(2):
                value = pad_ref[part, at, :].astype(jnp.float32)
                slope = 0.5 * (pltpu.roll(value, wide - 1, 1) - pltpu.roll(value, 1, 1))
                for k in range(wide // lanes):
                    cols = slice(k * lanes, (k + 1) * lanes)
                    planes[part, k, lower, :] = value[:, cols]
                    planes[2 + part, k, lower, :] = slope[:, cols]

    pairs = ((fwd_hbm, fwd_ref), (probe_hbm, probe_ref), (bwd_hbm, bwd_ref), (frames_hbm, frames_ref))
    loads = [pltpu.make_async_copy(source, target, local_sems.at[k]) for k, (source, target) in enumerate(pairs)]
    for load in loads:
        load.start()
    gather_halo(n_tile, n_pos, n // 2, x_hbm, pad_ref, send_sems, recv_sems, local_sems.at[4], convert)
    for load in loads:
        load.wait()

    @pl.loop(0, steps)
    def _(step):
        for b in range(batch):
            j = step * batch + b
            row, col = off_ref[0, j], off_ref[1, j]
            block, shift = col // lanes, col % lanes
            turn = (lanes - shift) % lanes
            for part in range(4):
                high = n + 8 if part < 2 else n
                first = row + 7 if part < 2 else row + 8
                target = patch.at[b, part] if part < 2 else slant.at[b, part - 2]
                keep = lax.broadcasted_iota(jnp.int32, (high, lanes), 1) < lanes - shift
                turned = [
                    pltpu.roll(planes[part, block + k, pl.ds(first, high), :], turn, 1) for k in range(blocks + 1)
                ]
                for k in range(blocks):
                    target[:, k * lanes : (k + 1) * lanes] = jnp.where(keep, turned[k], turned[k + 1])
            o_re, o_im = patch[b, 0, 1 : n + 1, :], patch[b, 1, 1 : n + 1, :]
            p_re, p_im = probe_ref[0], probe_ref[1]
            exits[b, :n, :] = (p_re * o_re - p_im * o_im).astype(jnp.bfloat16)
            exits[b, n:, :] = (p_re * o_im + p_im * o_re).astype(jnp.bfloat16)
        for b in range(batch):
            half = jnp.dot(fwd_ref[...], exits[b], preferred_element_type=jnp.float32)
            halves[b * n : (b + 1) * n, :n] = half[:n].astype(jnp.bfloat16)
            halves[b * n : (b + 1) * n, n:] = half[n:].astype(jnp.bfloat16)
        losses = []
        for b in range(batch):
            wave = jnp.dot(halves[b * n : (b + 1) * n, :], bwd_ref[...], preferred_element_type=jnp.float32)
            f_re, f_im = wave[:, :n], wave[:, n:]
            square = f_re * f_re + f_im * f_im
            keep_part = 1.0 - frames_ref[step * batch + b].astype(jnp.float32) * lax.rsqrt(jnp.maximum(square, 0.0625))
            losses.append(fold(square * (keep_part * keep_part)))
            resid[b, :n, :] = (f_re * keep_part).astype(jnp.bfloat16)
            resid[b, n:, :] = (f_im * keep_part).astype(jnp.bfloat16)
        for b in range(batch):
            back = jnp.dot(bwd_ref[...], resid[b], preferred_element_type=jnp.float32)
            inner[b * n : (b + 1) * n, :n] = back[:n].astype(jnp.bfloat16)
            inner[b * n : (b + 1) * n, n:] = back[n:].astype(jnp.bfloat16)
        for b in range(batch):
            j = step * batch + b
            wave = jnp.dot(inner[b * n : (b + 1) * n, :], fwd_ref[...], preferred_element_type=jnp.float32)
            g_re, g_im = wave[:, :n], wave[:, n:]
            p_re, p_im = probe_ref[0], probe_ref[1]
            q_re = g_re * p_re + g_im * p_im
            q_im = g_re * p_im - g_im * p_re
            d_re = patch[b, 0, 2 : n + 2, :] - patch[b, 0, 0:n, :]
            d_im = patch[b, 1, 2 : n + 2, :] - patch[b, 1, 0:n, :]
            by_row = fold(q_re * d_re - q_im * d_im) * 0.5
            by_col = fold(q_re * slant[b, 0] - q_im * slant[b, 1])
            for which, value in enumerate((by_row, by_col, losses[b] * (1.0 / (n * n)))):
                line = jnp.sum(value, axis=0, keepdims=True)
                short = line[:, :lanes]
                for k in range(1, blocks):
                    short = short + line[:, k * lanes : (k + 1) * lanes]
                sums[which, pl.ds(j, 1), :] = short

    count = sums.shape[1]
    diagonal = lax.broadcasted_iota(jnp.int32, (count, lanes), 0) == lax.broadcasted_iota(jnp.int32, (count, lanes), 1)
    lines = []
    for which in range(3):
        full = jnp.sum(sums[which], axis=1, keepdims=True)
        lines.append(jnp.sum(jnp.where(diagonal, full, 0.0), axis=0, keepdims=True))
    squares = jnp.sum(lines[0] * lines[0] + lines[1] * lines[1], axis=1, keepdims=True)
    line_ref[...] = jnp.broadcast_to(squares, (1, lanes))
    lines.append(shared_sum(n_tile, n_pos, line_ref, others, sum_sends, sum_recvs))
    out_ref[...] = jnp.concatenate(lines + [jnp.zeros((4, lanes), jnp.float32)], axis=0)


def refine(quarter, probe, frames, offsets, n_tile, n_pos):
    count, n, _ = frames.shape
    _, height, width = quarter.shape
    if count % BATCH or count > 128 or n % 128 or n_pos != 4 or height < n // 2:
        raise ValueError("unsupported sizes")
    forward, backward = dft_tables(n)
    tall, wide = height * n_pos + n, width + n
    steps = count // BATCH
    devices = n_tile * n_pos
    vmem, dma = pltpu.VMEM, pltpu.SemaphoreType.DMA
    anywhere = pl.BlockSpec(memory_space=pl.ANY)
    return pl.pallas_call(
        functools.partial(refine_kernel, BATCH, steps, n_tile, n_pos),
        out_shape=jax.ShapeDtypeStruct((8, 128), jnp.float32),
        in_specs=[pl.BlockSpec(memory_space=pltpu.SMEM)] + [anywhere] * 5,
        out_specs=pl.BlockSpec(memory_space=pltpu.VMEM),
        scratch_shapes=[
            vmem((2, tall, wide), jnp.bfloat16),
            vmem(probe.shape, jnp.float32),
            vmem(forward.shape, jnp.bfloat16),
            vmem(backward.shape, jnp.bfloat16),
            vmem(frames.shape, jnp.bfloat16),
            vmem((4, wide // 128, tall + 16, 128), jnp.float32),
            vmem((BATCH, 2, n + 8, n), jnp.float32),
            vmem((BATCH, 2, n, n), jnp.float32),
            vmem((BATCH, 2 * n, n), jnp.bfloat16),
            vmem((BATCH * n, 2 * n), jnp.bfloat16),
            vmem((BATCH, 2 * n, n), jnp.bfloat16),
            vmem((BATCH * n, 2 * n), jnp.bfloat16),
            vmem((3, count, 128), jnp.float32),
            dma((SENDS,)),
            dma((RECEIVES,)),
            dma((5,)),
            vmem((1, 128), jnp.float32),
            vmem((devices - 1, 1, 128), jnp.float32),
            dma((devices - 1,)),
            dma((devices - 1,)),
        ],
        compiler_params=pltpu.CompilerParams(
            vmem_limit_bytes=56 * 1024 * 1024, collective_id=0, has_side_effects=True
        ),
    )(offsets, quarter, probe, frames, forward, backward)


def scale_kernel(positions, lines_ref, shifts_ref, losses_ref):
    count = shifts_ref.shape[1]
    scale = jnp.sqrt(lines_ref[3:4, :] * (1.0 / positions) + 1e-06)
    shifts_ref[...] = (-lines_ref[0:2, :] / scale)[:, :count]
    losses_ref[...] = lines_ref[2:3, :count]


def normalise(lines, count, positions):
    block = pl.BlockSpec(memory_space=pltpu.VMEM)
    return pl.pallas_call(
        functools.partial(scale_kernel, positions),
        out_shape=(jax.ShapeDtypeStruct((2, count), jnp.float32), jax.ShapeDtypeStruct((1, count), jnp.float32)),
        in_specs=[block],
        out_specs=(block, block),
    )(lines)


def solution(mesh):
    n_tile, n_pos = mesh.shape["tile"], mesh.shape["pos"]

    def local(object_tiles, probe, frames, offsets):
        count = frames.shape[0]
        lines = refine(object_tiles[0], probe, frames, offsets, n_tile, n_pos)
        shifts, losses = normalise(lines, count, count * n_tile * n_pos)
        return shifts, losses[0]

    in_specs = (
        P("tile", None, "pos", None),
        P(),
        P(("tile", "pos"), None, None),
        P(None, ("tile", "pos")),
    )
    out_specs = (P(None, ("tile", "pos")), P(("tile", "pos")))
    return jax.shard_map(local, mesh=mesh, in_specs=in_specs, out_specs=out_specs, check_vma=False)
```

```python
import functools
import math

import jax
import jax.numpy as jnp
import numpy as np
from jax import lax
from jax.experimental import pallas as pl
from jax.experimental.pallas import tpu as pltpu
from jax.sharding import PartitionSpec as P

GC = 4
SENDS = 64
STOPS = 4
RECEIVES = 35
BATCH = 2
MESH_ID = pl.DeviceIdType.MESH


def dft_tables(length_n):
    indices = np.arange(length_n)
    products_mod = indices[:, None] * indices[None, :] % length_n
    angles = products_mod.astype(np.float32) * np.float32(2.0 * math.pi / length_n)
    factor = np.float32(1.0 / math.sqrt(length_n))
    cosine, sine = np.cos(angles) * factor, np.sin(angles) * factor
    forward = np.block([[cosine, sine], [-sine, cosine]])
    low = slice(0, length_n // 2)
    split = [np.block([[cosine[low, q::2], sine[low, q::2]], [-sine[low, q::2], cosine[low, q::2]]]) for q in range(2)]
    pieces = np.stack(split + [piece.T for piece in split])
    return [jnp.asarray(table, jnp.bfloat16) for table in (forward, forward.T, pieces)]


def gather_halo(n_tile, n_pos, margin, x_hbm, pad_ref, send_sems, recv_sems, alive, local_sem, convert):
    t, p = lax.axis_index("tile"), lax.axis_index("pos")
    _, quarter, width = x_hbm.shape
    rows = pad_ref.shape[1] - 2 * margin
    last = rows // quarter - 1
    c, r = t % GC, t // GC
    core, half = p % 2, p // 2
    near, far = p + 1 - 2 * core, p + 2 - 4 * half
    near_far = near + 2 - 4 * half
    west, east = c > 0, c < GC - 1
    north, south = r > 0, r < n_tile // GC - 1
    yes = p >= 0
    both = jnp.logical_and
    tall, wide = rows + 2 * margin, width + 2 * margin

    relatives = [(None, t, (p + k) % n_pos) for k in range(1, n_pos)] + [(west, t - 1, p), (east, t + 1, p)]
    relatives += [(north, t - GC, p), (north, t - GC, far), (south, t + GC, p), (south, t + GC, far)]
    ones = lambda cond: jnp.where(cond, 1, 0)
    count = n_pos - 1 + ones(west) + ones(east) + 2 * ones(north) + 2 * ones(south)

    def greet(semaphore):
        for cond, to_t, to_p in relatives:
            signal = functools.partial(
                pl.semaphore_signal, semaphore, inc=1, device_id=(to_t, to_p), device_id_type=MESH_ID
            )
            if cond is None:
                signal()
            else:
                pl.when(cond)(signal)

    barrier = pltpu.get_barrier_semaphore()
    greet(barrier)
    rounds, share = alive.shape[0], -(-alive.shape[0] // STOPS)

    def spread(stop):
        for k in range(stop * share, min((stop + 1) * share, rounds)):
            pl.semaphore_wait(alive.at[k], count)
            if k + 1 < rounds:
                greet(alive.at[k + 1])

    def block(q):
        return pl.ds(pl.multiple_of(margin + q * quarter, quarter), quarter)

    mine, its, nears, nears_far = block(p), block(far), block(near), block(near_far)
    above, below = slice(0, margin), slice(margin + rows, tall)
    top, bottom = slice(margin, 2 * margin), slice(rows, margin + rows)
    mid = slice(margin, margin + width)
    left, right = slice(0, margin), slice(margin + width, wide)
    first_cols, last_cols = slice(margin, 2 * margin), slice(width, margin + width)
    inner_cols = slice(2 * margin, width)
    strips = (first_cols, last_cols, inner_cols)
    sent = []

    def at(rows_at, cols_at):
        return pad_ref.at[:, rows_at, cols_at]

    own = pltpu.make_async_copy(x_hbm, at(mine, mid), local_sem)
    own.start()

    def zero(cond, rows_at, cols_at):
        @pl.when(cond)
        def _():
            part = at(rows_at, cols_at)
            part[...] = jnp.zeros(part.shape, part.dtype)

    zero(jnp.logical_not(west), slice(0, tall), left)
    zero(jnp.logical_not(east), slice(0, tall), right)
    zero(jnp.logical_not(north), above, slice(0, wide))
    zero(jnp.logical_not(south), below, slice(0, wide))

    def copy(index, src, dst, to_t, to_p, send_index):
        return pltpu.make_async_remote_copy(
            src_ref=src,
            dst_ref=dst,
            send_sem=send_sems.at[send_index],
            recv_sem=recv_sems.at[index],
            device_id=(to_t, to_p),
            device_id_type=MESH_ID,
        )

    def send(cond, index, src, dst, to_t, to_p):
        made = copy(index, src, dst, to_t, to_p, len(sent))
        sent.append((cond, made))

        @pl.when(cond)
        def _():
            made.start()

    def receive(cond, index, dst):
        @pl.when(cond)
        def _():
            copy(index, dst, dst, t, near, 0).wait_recv()

    own.wait()
    pl.semaphore_wait(barrier, count)
    if rounds:
        greet(alive.at[0])

    up, down = both(p == 0, north), both(p == last, south)
    native = jnp.logical_or(up, down)
    buddy = jnp.logical_or(both(near == 0, north), both(near == last, south))
    far_up, far_down = both(far == 0, north), both(far == last, south)
    relays = jnp.logical_or(far_up, far_down)
    plain = jnp.logical_not(jnp.logical_or(native, buddy))
    send(east, 0, at(mine, last_cols), at(mine, left), t + 1, p)
    send(west, 1, at(mine, first_cols), at(mine, right), t - 1, p)
    vertical = ((up, top, below, t - GC, 6), (down, bottom, above, t + GC, 9))
    send(native, 4, at(mine, inner_cols), at(mine, inner_cols), t, far)
    for cond, src, dst, to_t, base in vertical:
        for k in range(2):
            send(cond, base + k, at(src, strips[k]), at(dst, strips[k]), to_t, p)
            send(cond, base + k, at(src, strips[k]), at(dst, strips[k]), to_t, far)
        send(cond, base + 2, at(src, strips[2]), at(dst, strips[2]), to_t, p)
    for k in range(2):
        send(native, 2 + k, at(mine, strips[k]), at(mine, strips[k]), t, far)
    for k in range(3):
        send(plain, 2 + k, at(mine, strips[k]), at(mine, strips[k]), t, far)
    send(yes, 5, at(mine, mid), at(mine, mid), t, near)

    receive(west, 0, at(mine, left))
    receive(east, 1, at(mine, right))
    for k in range(3):
        send(buddy, 2 + k, at(mine, strips[k]), at(mine, strips[k]), t, far)
    send(west, 15, at(mine, left), at(mine, left), t, near)
    send(east, 16, at(mine, right), at(mine, right), t, near)
    spread(0)
    receive(relays, 4, at(its, inner_cols))
    send(far_up, 8, at(top, inner_cols), at(below, inner_cols), t - GC, p)
    send(far_down, 11, at(bottom, inner_cols), at(above, inner_cols), t + GC, p)
    pl.when(jnp.logical_not(north))(lambda: convert(0, margin))
    pl.when(jnp.logical_not(south))(lambda: convert(margin + rows, margin))
    receive(yes, 2, at(its, first_cols))
    send(west, 13, at(its, first_cols), at(its, right), t - 1, p)
    receive(yes, 3, at(its, last_cols))
    send(east, 12, at(its, last_cols), at(its, left), t + 1, p)
    send(yes, 14, at(its, first_cols), at(its, first_cols), t, near)
    send(yes, 33, at(its, last_cols), at(its, last_cols), t, near)
    convert(margin + p * quarter, quarter)
    spread(1)

    halos = ((both(south, core == 0), below, 6, 19, 25), (both(north, core == 1), above, 9, 22, 27))
    for cond, area, base, shared, corner in halos:
        receive(cond, base, at(area, first_cols))
        send(both(cond, west), corner, at(area, first_cols), at(area, right), t - 1, p)
        receive(cond, base + 1, at(area, last_cols))
        send(both(cond, east), corner + 1, at(area, last_cols), at(area, left), t + 1, p)
        send(cond, shared, at(area, first_cols), at(area, first_cols), t, near)
        send(cond, shared + 1, at(area, last_cols), at(area, last_cols), t, near)

    receive(yes, 5, at(nears, mid))
    receive(west, 15, at(nears, left))
    receive(east, 16, at(nears, right))
    convert(margin + near * quarter, quarter)
    spread(2)

    for cond, area, base, shared, corner in halos:
        receive(cond, base + 2, at(area, inner_cols))
        send(cond, shared + 2, at(area, inner_cols), at(area, inner_cols), t, near)
    receive(jnp.logical_not(relays), 4, at(its, inner_cols))
    send(yes, 34, at(its, inner_cols), at(its, inner_cols), t, near)
    receive(east, 13, at(its, right))
    send(east, 18, at(its, right), at(its, right), t, near)
    receive(west, 12, at(its, left))
    send(west, 17, at(its, left), at(its, left), t, near)
    for cond, area, base, shared, corner in halos:
        receive(both(cond, east), corner, at(area, right))
        send(both(cond, east), corner + 4, at(area, right), at(area, right), t, near)
        receive(both(cond, west), corner + 1, at(area, left))
        send(both(cond, west), corner + 5, at(area, left), at(area, left), t, near)
    convert(margin + far * quarter, quarter)
    spread(3)

    others = ((both(south, core == 1), below, 19, 25), (both(north, core == 0), above, 22, 27))
    for cond, area, shared, corner in others:
        for k in range(3):
            receive(cond, shared + k, at(area, strips[k]))
        receive(both(cond, east), corner + 4, at(area, right))
        receive(both(cond, west), corner + 5, at(area, left))
    pl.when(north)(lambda: convert(0, margin))
    pl.when(south)(lambda: convert(margin + rows, margin))
    receive(yes, 14, at(nears_far, first_cols))
    receive(yes, 33, at(nears_far, last_cols))
    receive(west, 17, at(nears_far, left))
    receive(east, 18, at(nears_far, right))
    receive(yes, 34, at(nears_far, inner_cols))
    convert(margin + near_far * quarter, quarter)
    for cond, made in sent:
        @pl.when(cond)
        def _():
            made.wait_send()


def shared_sum(n_tile, n_pos, mine_ref, others, send_sems, recv_sems):
    me = lax.axis_index("tile") * n_pos + lax.axis_index("pos")
    count = n_tile * n_pos
    copies = []
    for k in range(1, count):
        other = lax.rem(me + k, count)
        made = pltpu.make_async_remote_copy(
            src_ref=mine_ref,
            dst_ref=others.at[k - 1],
            send_sem=send_sems.at[k - 1],
            recv_sem=recv_sems.at[k - 1],
            device_id=(other // n_pos, other % n_pos),
            device_id_type=MESH_ID,
        )
        made.start()
        copies.append(made)
    for made in copies:
        made.wait()
    return jnp.sum(others[...], axis=0) + mine_ref[...]


def fold(value):
    return jnp.sum(value.reshape(-1, 8, value.shape[-1]), axis=0)


def refine_kernel(
    batch, steps, n_tile, n_pos, off_ref, x_hbm, probe_hbm, frames_hbm, fwd_hbm, bwd_hbm, pieces_hbm, out_ref,
    pad_ref, probe_ref, fwd_ref, bwd_ref, pieces_ref, frames_ref, planes, patch, turned, exits, halves, resid, inner,
    sums, send_sems, recv_sems, alive, local_sems, line_ref, others, sum_sends, sum_recvs,
):
    n = probe_ref.shape[2]
    h = n // 2
    tall, wide = pad_ref.shape[1], pad_ref.shape[2]
    lanes = 128

    def convert(first, height):
        @pl.loop(0, height // 32)
        def _(i):
            at = pl.ds(pl.multiple_of(first + i * 32, 32), 32)
            lower = pl.ds(pl.multiple_of(first + i * 32 + 8, 8), 32)
            for part in range(2):
                value = pad_ref[part, at, :].astype(jnp.float32)
                slope = 0.5 * (pltpu.roll(value, wide - 1, 1) - pltpu.roll(value, 1, 1))
                for k in range(wide // lanes):
                    cols = slice(k * lanes, (k + 1) * lanes)
                    planes[part, k, lower, :] = value[:, cols]
                    planes[2 + part, k, lower, :] = slope[:, cols]

    pairs = [(fwd_hbm, fwd_ref), (bwd_hbm, bwd_ref), (pieces_hbm, pieces_ref), (frames_hbm, frames_ref)]
    for part in range(2):
        for k in range(2):
            pairs.append((probe_hbm.at[part, :, pl.ds(k * lanes, lanes)], probe_ref.at[part, k]))
    loads = [pltpu.make_async_copy(source, target, local_sems.at[k + 1]) for k, (source, target) in enumerate(pairs)]
    for load in loads:
        load.start()
    gather_halo(n_tile, n_pos, n // 2, x_hbm, pad_ref, send_sems, recv_sems, alive, local_sems.at[0], convert)
    for load in loads:
        load.wait()

    lane = lax.broadcasted_iota(jnp.int32, (1, lanes), 1)

    def place(step, b):
        j = step * batch + b
        row, col = off_ref[0, j], off_ref[1, j]
        return row, col // lanes, col % lanes

    def extract(step, b, buf):
        row, block, shift = place(step, b)
        keep = lane >= shift
        for part in range(2):
            for seq in range(2):
                rows = pl.ds(row + 7 + seq, h + 8, stride=2)
                patch[buf, b, part, seq] = jnp.where(keep, planes[part, block, rows, :], planes[part, block + 2, rows, :])
        for q in range(2):
            rows = pl.ds(row + 8 + q, h, stride=2)
            for part in range(2):
                ends = [pltpu.roll(probe_ref[part, k, pl.ds(q, h, stride=2), :], shift, 1) for k in range(2)]
                turned[buf, b, part, q, 0] = jnp.where(keep, ends[0], ends[1])
                turned[buf, b, part, q, 1] = jnp.where(keep, ends[1], ends[0])
            for k in range(2):
                cols = slice(k * lanes, (k + 1) * lanes)
                if k == 0:
                    o_re, o_im = (patch[buf, b, part, 1 - q, q : q + h, :] for part in range(2))
                else:
                    o_re, o_im = (planes[part, block + 1, rows, :] for part in range(2))
                p_re, p_im = turned[buf, b, 0, q, k], turned[buf, b, 1, q, k]
                exits[b, q, :h, cols] = (p_re * o_re - p_im * o_im).astype(jnp.bfloat16)
                exits[b, q, h:, cols] = (p_re * o_im + p_im * o_re).astype(jnp.bfloat16)

    def along_rows(b):
        evens = jnp.dot(pieces_ref[0], exits[b, 0], preferred_element_type=jnp.float32)
        odds = jnp.dot(pieces_ref[1], exits[b, 1], preferred_element_type=jnp.float32)
        plus, minus = (evens + odds).astype(jnp.bfloat16), (evens - odds).astype(jnp.bfloat16)
        halves[b, :h, :n], halves[b, :h, n:] = plus[:h], plus[h:]
        halves[b, h:, :n], halves[b, h:, n:] = minus[:h], minus[h:]

    def residual(step, b):
        wave = jnp.dot(halves[b], bwd_ref[...], preferred_element_type=jnp.float32)
        f_re, f_im = wave[:, :n], wave[:, n:]
        square = f_re * f_re + f_im * f_im
        frame = frames_ref[step * batch + b].astype(jnp.float32)
        keep_part = 1.0 - frame * lax.rsqrt(jnp.maximum(square, 0.0625))
        r_re, r_im = f_re * keep_part, f_im * keep_part
        resid[b, 0, :h, :] = (r_re[:h] + r_re[h:]).astype(jnp.bfloat16)
        resid[b, 0, h:, :] = (r_im[:h] + r_im[h:]).astype(jnp.bfloat16)
        resid[b, 1, :h, :] = (r_re[:h] - r_re[h:]).astype(jnp.bfloat16)
        resid[b, 1, h:, :] = (r_im[:h] - r_im[h:]).astype(jnp.bfloat16)
        loss = fold(square * (keep_part * keep_part)) * (1.0 / (n * n))
        sums[2, pl.ds(step * batch + b, 1), :] = jnp.sum(loss[:, :lanes] + loss[:, lanes:], axis=0, keepdims=True)

    def back_rows(b):
        for q in range(2):
            back = jnp.dot(pieces_ref[2 + q], resid[b, q], preferred_element_type=jnp.float32).astype(jnp.bfloat16)
            inner[b, q * h : (q + 1) * h, :n] = back[:h]
            inner[b, q * h : (q + 1) * h, n:] = back[h:]

    def slopes(step, b, buf):
        row, block, shift = place(step, b)
        keep = lane >= shift
        wave = jnp.dot(inner[b], fwd_ref[...], preferred_element_type=jnp.float32)
        by_row, by_col = 0.0, 0.0
        for q in range(2):
            rows = pl.ds(row + 8 + q, h, stride=2)
            before, after = pl.ds(row + 7 + q, h, stride=2), pl.ds(row + 9 + q, h, stride=2)
            for k in range(2):
                g_re = wave[q * h : (q + 1) * h, k * lanes : (k + 1) * lanes]
                g_im = wave[q * h : (q + 1) * h, n + k * lanes : n + (k + 1) * lanes]
                p_re, p_im = turned[buf, b, 0, q, k], turned[buf, b, 1, q, k]
                q_re = g_re * p_re + g_im * p_im
                q_im = g_re * p_im - g_im * p_re
                if k == 0:
                    d_re, d_im = (
                        patch[buf, b, part, q, 1 : h + 1, :] - patch[buf, b, part, q, 0:h, :] for part in range(2)
                    )
                    s_re, s_im = (
                        jnp.where(keep, planes[2 + part, block, rows, :], planes[2 + part, block + 2, rows, :])
                        for part in range(2)
                    )
                else:
                    d_re, d_im = (
                        planes[part, block + 1, after, :] - planes[part, block + 1, before, :] for part in range(2)
                    )
                    s_re, s_im = (planes[2 + part, block + 1, rows, :] for part in range(2))
                by_row = by_row + fold(q_re * d_re - q_im * d_im)
                by_col = by_col + fold(q_re * s_re - q_im * s_im)
        for which, value in enumerate((0.5 * by_row, by_col)):
            sums[which, pl.ds(step * batch + b, 1), :] = jnp.sum(value, axis=0, keepdims=True)

    def advance(step, buf):
        later = jnp.minimum(step + 1, steps - 1)
        for b in range(batch):
            along_rows(b)
        for b in range(batch // 2):
            extract(later, b, 1 - buf)
        for b in range(batch):
            residual(step, b)
        for b in range(batch):
            back_rows(b)
        for b in range(batch // 2, batch):
            extract(later, b, 1 - buf)
        for b in range(batch):
            slopes(step, b, buf)

    for b in range(batch):
        extract(0, b, 0)

    @pl.loop(0, steps // 2)
    def _(pair):
        advance(2 * pair, 0)
        advance(2 * pair + 1, 1)

    count = sums.shape[1]
    diagonal = lax.broadcasted_iota(jnp.int32, (count, lanes), 0) == lax.broadcasted_iota(jnp.int32, (count, lanes), 1)
    lines = []
    for which in range(3):
        full = jnp.sum(sums[which], axis=1, keepdims=True)
        lines.append(jnp.sum(jnp.where(diagonal, full, 0.0), axis=0, keepdims=True))
    squares = jnp.sum(lines[0] * lines[0] + lines[1] * lines[1], axis=1, keepdims=True)
    line_ref[...] = jnp.broadcast_to(squares, (1, lanes))
    lines.append(shared_sum(n_tile, n_pos, line_ref, others, sum_sends, sum_recvs))
    out_ref[...] = jnp.concatenate(lines + [jnp.zeros((4, lanes), jnp.float32)], axis=0)


def refine(quarter, probe, frames, offsets, n_tile, n_pos):
    count, n, _ = frames.shape
    _, height, width = quarter.shape
    if count % (2 * BATCH) or count > 128 or n != 2 * 128 or n_pos != 4 or height < n // 2:
        raise ValueError("unsupported sizes")
    forward, backward, pieces = dft_tables(n)
    tall, wide = height * n_pos + n, width + n
    steps = count // BATCH
    devices = n_tile * n_pos
    vmem, dma = pltpu.VMEM, pltpu.SemaphoreType.DMA
    anywhere = pl.BlockSpec(memory_space=pl.ANY)
    return pl.pallas_call(
        functools.partial(refine_kernel, BATCH, steps, n_tile, n_pos),
        out_shape=jax.ShapeDtypeStruct((8, 128), jnp.float32),
        in_specs=[pl.BlockSpec(memory_space=pltpu.SMEM)] + [anywhere] * 6,
        out_specs=pl.BlockSpec(memory_space=pltpu.VMEM),
        scratch_shapes=[
            vmem((2, tall, wide), jnp.bfloat16),
            vmem((2, 2, n, 128), jnp.float32),
            vmem(forward.shape, jnp.bfloat16),
            vmem(backward.shape, jnp.bfloat16),
            vmem(pieces.shape, jnp.bfloat16),
            vmem(frames.shape, jnp.bfloat16),
            vmem((4, wide // 128, tall + 32, 128), jnp.float32),
            vmem((2, BATCH, 2, 2, n // 2 + 8, 128), jnp.float32),
            vmem((2, BATCH, 2, 2, 2, n // 2, 128), jnp.float32),
            vmem((BATCH, 2, n, n), jnp.bfloat16),
            vmem((BATCH, n, 2 * n), jnp.bfloat16),
            vmem((BATCH, 2, n, n), jnp.bfloat16),
            vmem((BATCH, n, 2 * n), jnp.bfloat16),
            vmem((3, count, 128), jnp.float32),
            dma((SENDS,)),
            dma((RECEIVES,)),
            pltpu.SemaphoreType.REGULAR((GC + n_tile // GC - 2,)),
            dma((9,)),
            vmem((1, 128), jnp.float32),
            vmem((devices - 1, 1, 128), jnp.float32),
            dma((devices - 1,)),
            dma((devices - 1,)),
        ],
        compiler_params=pltpu.CompilerParams(
            vmem_limit_bytes=56 * 1024 * 1024, collective_id=0, has_side_effects=True
        ),
    )(offsets, quarter, probe, frames, forward, backward, pieces)


def scale_kernel(positions, lines_ref, shifts_ref, losses_ref):
    count = shifts_ref.shape[1]
    scale = jnp.sqrt(lines_ref[3:4, :] * (1.0 / positions) + 1e-06)
    shifts_ref[...] = (-lines_ref[0:2, :] / scale)[:, :count]
    losses_ref[...] = lines_ref[2:3, :count]


def normalise(lines, count, positions):
    block = pl.BlockSpec(memory_space=pltpu.VMEM)
    return pl.pallas_call(
        functools.partial(scale_kernel, positions),
        out_shape=(jax.ShapeDtypeStruct((2, count), jnp.float32), jax.ShapeDtypeStruct((1, count), jnp.float32)),
        in_specs=[block],
        out_specs=(block, block),
    )(lines)


def solution(mesh):
    n_tile, n_pos = mesh.shape["tile"], mesh.shape["pos"]

    def local(object_tiles, probe, frames, offsets):
        count = frames.shape[0]
        lines = refine(object_tiles[0], probe, frames, offsets, n_tile, n_pos)
        shifts, losses = normalise(lines, count, count * n_tile * n_pos)
        return shifts, losses[0]

    in_specs = (
        P("tile", None, "pos", None),
        P(),
        P(("tile", "pos"), None, None),
        P(None, ("tile", "pos")),
    )
    out_specs = (P(None, ("tile", "pos")), P(("tile", "pos")))
    return jax.shard_map(local, mesh=mesh, in_specs=in_specs, out_specs=out_specs, check_vma=False)
```

```python
import functools
import math

import jax
import jax.numpy as jnp
import numpy as np
from jax import lax
from jax.experimental import pallas as pl
from jax.experimental.pallas import tpu as pltpu
from jax.sharding import PartitionSpec as P

GC = 4
SENDS = 64
STOPS = 4
RECEIVES = 35
BATCH = 2
MESH_ID = pl.DeviceIdType.MESH


def dft_tables(length_n):
    indices = np.arange(length_n)
    products_mod = indices[:, None] * indices[None, :] % length_n
    angles = products_mod.astype(np.float32) * np.float32(2.0 * math.pi / length_n)
    factor = np.float32(1.0 / math.sqrt(length_n))
    cosine, sine = np.cos(angles) * factor, np.sin(angles) * factor
    forward = np.block([[cosine, sine], [-sine, cosine]])
    low = slice(0, length_n // 2)
    split = [np.block([[cosine[low, q::2], sine[low, q::2]], [-sine[low, q::2], cosine[low, q::2]]]) for q in range(2)]
    pieces = np.stack(split + [piece.T for piece in split])
    return [jnp.asarray(table, jnp.bfloat16) for table in (forward, forward.T, pieces)]


def gather_halo(n_tile, n_pos, margin, x_hbm, pad_ref, send_sems, recv_sems, alive, local_sem, loads, convert):
    t, p = lax.axis_index("tile"), lax.axis_index("pos")
    _, quarter, width = x_hbm.shape
    rows = pad_ref.shape[1] - 2 * margin
    last = rows // quarter - 1
    c, r = t % GC, t // GC
    core, half = p % 2, p // 2
    near, far = p + 1 - 2 * core, p + 2 - 4 * half
    near_far = near + 2 - 4 * half
    west, east = c > 0, c < GC - 1
    north, south = r > 0, r < n_tile // GC - 1
    yes = p >= 0
    both = jnp.logical_and
    tall, wide = rows + 2 * margin, width + 2 * margin

    relatives = [(None, t, (p + k) % n_pos) for k in range(1, n_pos)] + [(west, t - 1, p), (east, t + 1, p)]
    relatives += [(north, t - GC, p), (north, t - GC, far), (south, t + GC, p), (south, t + GC, far)]
    ones = lambda cond: jnp.where(cond, 1, 0)
    count = n_pos - 1 + ones(west) + ones(east) + 2 * ones(north) + 2 * ones(south)

    mine = pl.ds(pl.multiple_of(margin + p * quarter, quarter), quarter)
    own = pltpu.make_async_copy(x_hbm, pad_ref.at[:, mine, margin : margin + width], local_sem)
    own.start()

    def greet(semaphore):
        for cond, to_t, to_p in relatives:
            signal = functools.partial(
                pl.semaphore_signal, semaphore, inc=1, device_id=(to_t, to_p), device_id_type=MESH_ID
            )
            if cond is None:
                signal()
            else:
                pl.when(cond)(signal)

    barrier = pltpu.get_barrier_semaphore()
    greet(barrier)
    for load in loads:
        load.start()
    rounds, share = alive.shape[0], -(-alive.shape[0] // STOPS)

    def spread(stop):
        for k in range(stop * share, min((stop + 1) * share, rounds)):
            pl.semaphore_wait(alive.at[k], count)
            if k + 1 < rounds:
                greet(alive.at[k + 1])

    def block(q):
        return pl.ds(pl.multiple_of(margin + q * quarter, quarter), quarter)

    its, nears, nears_far = block(far), block(near), block(near_far)
    above, below = slice(0, margin), slice(margin + rows, tall)
    top, bottom = slice(margin, 2 * margin), slice(rows, margin + rows)
    mid = slice(margin, margin + width)
    left, right = slice(0, margin), slice(margin + width, wide)
    first_cols, last_cols = slice(margin, 2 * margin), slice(width, margin + width)
    inner_cols = slice(2 * margin, width)
    strips = (first_cols, last_cols, inner_cols)
    sent = []

    def at(rows_at, cols_at):
        return pad_ref.at[:, rows_at, cols_at]

    def zero(cond, rows_at, cols_at):
        @pl.when(cond)
        def _():
            part = at(rows_at, cols_at)
            part[...] = jnp.zeros(part.shape, part.dtype)

    zero(jnp.logical_not(west), slice(0, tall), left)
    zero(jnp.logical_not(east), slice(0, tall), right)
    zero(jnp.logical_not(north), above, slice(0, wide))
    zero(jnp.logical_not(south), below, slice(0, wide))

    def copy(index, src, dst, to_t, to_p, send_index):
        return pltpu.make_async_remote_copy(
            src_ref=src,
            dst_ref=dst,
            send_sem=send_sems.at[send_index],
            recv_sem=recv_sems.at[index],
            device_id=(to_t, to_p),
            device_id_type=MESH_ID,
        )

    def send(cond, index, src, dst, to_t, to_p):
        made = copy(index, src, dst, to_t, to_p, len(sent))
        sent.append((cond, made))

        @pl.when(cond)
        def _():
            made.start()

    def receive(cond, index, dst):
        @pl.when(cond)
        def _():
            copy(index, dst, dst, t, near, 0).wait_recv()

    own.wait()
    pl.semaphore_wait(barrier, count)
    if rounds:
        greet(alive.at[0])

    up, down = both(p == 0, north), both(p == last, south)
    native = jnp.logical_or(up, down)
    buddy = jnp.logical_or(both(near == 0, north), both(near == last, south))
    far_up, far_down = both(far == 0, north), both(far == last, south)
    relays = jnp.logical_or(far_up, far_down)
    plain = jnp.logical_not(jnp.logical_or(native, buddy))
    send(east, 0, at(mine, last_cols), at(mine, left), t + 1, p)
    send(west, 1, at(mine, first_cols), at(mine, right), t - 1, p)
    vertical = ((up, top, below, t - GC, 6), (down, bottom, above, t + GC, 9))
    send(native, 4, at(mine, inner_cols), at(mine, inner_cols), t, far)
    for cond, src, dst, to_t, base in vertical:
        for k in range(2):
            send(cond, base + k, at(src, strips[k]), at(dst, strips[k]), to_t, p)
            send(cond, base + k, at(src, strips[k]), at(dst, strips[k]), to_t, far)
        send(cond, base + 2, at(src, strips[2]), at(dst, strips[2]), to_t, p)
    for k in range(2):
        send(native, 2 + k, at(mine, strips[k]), at(mine, strips[k]), t, far)
    for k in range(3):
        send(plain, 2 + k, at(mine, strips[k]), at(mine, strips[k]), t, far)
    send(yes, 5, at(mine, mid), at(mine, mid), t, near)

    receive(west, 0, at(mine, left))
    receive(east, 1, at(mine, right))
    for k in range(3):
        send(buddy, 2 + k, at(mine, strips[k]), at(mine, strips[k]), t, far)
    send(west, 15, at(mine, left), at(mine, left), t, near)
    send(east, 16, at(mine, right), at(mine, right), t, near)
    spread(0)
    receive(relays, 4, at(its, inner_cols))
    send(far_up, 8, at(top, inner_cols), at(below, inner_cols), t - GC, p)
    send(far_down, 11, at(bottom, inner_cols), at(above, inner_cols), t + GC, p)
    pl.when(jnp.logical_not(north))(lambda: convert(0, margin))
    pl.when(jnp.logical_not(south))(lambda: convert(margin + rows, margin))
    receive(yes, 2, at(its, first_cols))
    send(west, 13, at(its, first_cols), at(its, right), t - 1, p)
    receive(yes, 3, at(its, last_cols))
    send(east, 12, at(its, last_cols), at(its, left), t + 1, p)
    send(yes, 14, at(its, first_cols), at(its, first_cols), t, near)
    send(yes, 33, at(its, last_cols), at(its, last_cols), t, near)
    convert(margin + p * quarter, quarter)
    spread(1)

    halos = ((both(south, core == 0), below, 6, 19, 25), (both(north, core == 1), above, 9, 22, 27))
    for cond, area, base, shared, corner in halos:
        receive(cond, base, at(area, first_cols))
        send(both(cond, west), corner, at(area, first_cols), at(area, right), t - 1, p)
        receive(cond, base + 1, at(area, last_cols))
        send(both(cond, east), corner + 1, at(area, last_cols), at(area, left), t + 1, p)
        send(cond, shared, at(area, first_cols), at(area, first_cols), t, near)
        send(cond, shared + 1, at(area, last_cols), at(area, last_cols), t, near)

    receive(yes, 5, at(nears, mid))
    receive(west, 15, at(nears, left))
    receive(east, 16, at(nears, right))
    convert(margin + near * quarter, quarter)
    spread(2)

    for cond, area, base, shared, corner in halos:
        receive(cond, base + 2, at(area, inner_cols))
        send(cond, shared + 2, at(area, inner_cols), at(area, inner_cols), t, near)
    receive(jnp.logical_not(relays), 4, at(its, inner_cols))
    send(yes, 34, at(its, inner_cols), at(its, inner_cols), t, near)
    receive(east, 13, at(its, right))
    send(east, 18, at(its, right), at(its, right), t, near)
    receive(west, 12, at(its, left))
    send(west, 17, at(its, left), at(its, left), t, near)
    for cond, area, base, shared, corner in halos:
        receive(both(cond, east), corner, at(area, right))
        send(both(cond, east), corner + 4, at(area, right), at(area, right), t, near)
        receive(both(cond, west), corner + 1, at(area, left))
        send(both(cond, west), corner + 5, at(area, left), at(area, left), t, near)
    convert(margin + far * quarter, quarter)
    spread(3)

    others = ((both(south, core == 1), below, 19, 25), (both(north, core == 0), above, 22, 27))
    for cond, area, shared, corner in others:
        for k in range(3):
            receive(cond, shared + k, at(area, strips[k]))
        receive(both(cond, east), corner + 4, at(area, right))
        receive(both(cond, west), corner + 5, at(area, left))
    pl.when(north)(lambda: convert(0, margin))
    pl.when(south)(lambda: convert(margin + rows, margin))
    receive(yes, 14, at(nears_far, first_cols))
    receive(yes, 33, at(nears_far, last_cols))
    receive(west, 17, at(nears_far, left))
    receive(east, 18, at(nears_far, right))
    receive(yes, 34, at(nears_far, inner_cols))
    convert(margin + near_far * quarter, quarter)
    for cond, made in sent:
        @pl.when(cond)
        def _():
            made.wait_send()


def shared_sum(n_tile, n_pos, mine_ref, others, send_sems, recv_sems):
    me = lax.axis_index("tile") * n_pos + lax.axis_index("pos")
    count = n_tile * n_pos
    copies = []
    for k in range(1, count):
        other = lax.rem(me + k, count)
        made = pltpu.make_async_remote_copy(
            src_ref=mine_ref,
            dst_ref=others.at[k - 1],
            send_sem=send_sems.at[k - 1],
            recv_sem=recv_sems.at[k - 1],
            device_id=(other // n_pos, other % n_pos),
            device_id_type=MESH_ID,
        )
        made.start()
        copies.append(made)
    for made in copies:
        made.wait()
    return jnp.sum(others[...], axis=0) + mine_ref[...]


def fold(value):
    return jnp.sum(value.reshape(-1, 8, value.shape[-1]), axis=0)


def refine_kernel(
    batch, steps, n_tile, n_pos, off_hbm, x_hbm, probe_hbm, frames_hbm, fwd_hbm, bwd_hbm, pieces_hbm, out_ref,
    off_ref, pad_ref, probe_ref, fwd_ref, bwd_ref, pieces_ref, frames_ref, planes, patch, turned, exits, halves, resid, inner,
    sums, send_sems, recv_sems, alive, local_sems, line_ref, others, sum_sends, sum_recvs,
):
    n = probe_ref.shape[2]
    h = n // 2
    tall, wide = pad_ref.shape[1], pad_ref.shape[2]
    lanes = 128

    def convert(first, height):
        @pl.loop(0, height // 32)
        def _(i):
            at = pl.ds(pl.multiple_of(first + i * 32, 32), 32)
            lower = pl.ds(pl.multiple_of(first + i * 32 + 8, 8), 32)
            for part in range(2):
                value = pad_ref[part, at, :].astype(jnp.float32)
                slope = 0.5 * (pltpu.roll(value, wide - 1, 1) - pltpu.roll(value, 1, 1))
                for k in range(wide // lanes):
                    cols = slice(k * lanes, (k + 1) * lanes)
                    planes[part, k, lower, :] = value[:, cols]
                    planes[2 + part, k, lower, :] = slope[:, cols]

    pairs = [(off_hbm, off_ref), (fwd_hbm, fwd_ref), (bwd_hbm, bwd_ref), (pieces_hbm, pieces_ref), (frames_hbm, frames_ref)]
    for part in range(2):
        for k in range(2):
            pairs.append((probe_hbm.at[part, :, pl.ds(k * lanes, lanes)], probe_ref.at[part, k]))
    loads = [pltpu.make_async_copy(source, target, local_sems.at[k + 1]) for k, (source, target) in enumerate(pairs)]
    gather_halo(n_tile, n_pos, n // 2, x_hbm, pad_ref, send_sems, recv_sems, alive, local_sems.at[0], loads, convert)
    for load in loads:
        load.wait()

    lane = lax.broadcasted_iota(jnp.int32, (1, lanes), 1)

    def place(step, b):
        j = step * batch + b
        row, col = off_ref[0, j], off_ref[1, j]
        return row, col // lanes, col % lanes

    def extract(step, b, buf):
        row, block, shift = place(step, b)
        keep = lane >= shift
        for part in range(2):
            for seq in range(2):
                rows = pl.ds(row + 7 + seq, h + 8, stride=2)
                patch[buf, b, part, seq] = jnp.where(keep, planes[part, block, rows, :], planes[part, block + 2, rows, :])
        for q in range(2):
            rows = pl.ds(row + 8 + q, h, stride=2)
            for part in range(2):
                ends = [pltpu.roll(probe_ref[part, k, pl.ds(q, h, stride=2), :], shift, 1) for k in range(2)]
                turned[buf, b, part, q, 0] = jnp.where(keep, ends[0], ends[1])
                turned[buf, b, part, q, 1] = jnp.where(keep, ends[1], ends[0])
            for k in range(2):
                cols = slice(k * lanes, (k + 1) * lanes)
                if k == 0:
                    o_re, o_im = (patch[buf, b, part, 1 - q, q : q + h, :] for part in range(2))
                else:
                    o_re, o_im = (planes[part, block + 1, rows, :] for part in range(2))
                p_re, p_im = turned[buf, b, 0, q, k], turned[buf, b, 1, q, k]
                exits[b, q, :h, cols] = (p_re * o_re - p_im * o_im).astype(jnp.bfloat16)
                exits[b, q, h:, cols] = (p_re * o_im + p_im * o_re).astype(jnp.bfloat16)

    def along_rows(b):
        evens = jnp.dot(pieces_ref[0], exits[b, 0], preferred_element_type=jnp.float32)
        odds = jnp.dot(pieces_ref[1], exits[b, 1], preferred_element_type=jnp.float32)
        plus, minus = (evens + odds).astype(jnp.bfloat16), (evens - odds).astype(jnp.bfloat16)
        halves[b, :h, :n], halves[b, :h, n:] = plus[:h], plus[h:]
        halves[b, h:, :n], halves[b, h:, n:] = minus[:h], minus[h:]

    def residual(step, b):
        wave = jnp.dot(halves[b], bwd_ref[...], preferred_element_type=jnp.float32)
        f_re, f_im = wave[:, :n], wave[:, n:]
        square = f_re * f_re + f_im * f_im
        frame = frames_ref[step * batch + b].astype(jnp.float32)
        keep_part = 1.0 - frame * lax.rsqrt(jnp.maximum(square, 0.0625))
        r_re, r_im = f_re * keep_part, f_im * keep_part
        resid[b, 0, :h, :] = (r_re[:h] + r_re[h:]).astype(jnp.bfloat16)
        resid[b, 0, h:, :] = (r_im[:h] + r_im[h:]).astype(jnp.bfloat16)
        resid[b, 1, :h, :] = (r_re[:h] - r_re[h:]).astype(jnp.bfloat16)
        resid[b, 1, h:, :] = (r_im[:h] - r_im[h:]).astype(jnp.bfloat16)
        loss = fold(square * (keep_part * keep_part)) * (1.0 / (n * n))
        sums[2, pl.ds(step * batch + b, 1), :] = jnp.sum(loss[:, :lanes] + loss[:, lanes:], axis=0, keepdims=True)

    def back_rows(b):
        for q in range(2):
            back = jnp.dot(pieces_ref[2 + q], resid[b, q], preferred_element_type=jnp.float32).astype(jnp.bfloat16)
            inner[b, q * h : (q + 1) * h, :n] = back[:h]
            inner[b, q * h : (q + 1) * h, n:] = back[h:]

    def slopes(step, b, buf):
        row, block, shift = place(step, b)
        keep = lane >= shift
        wave = jnp.dot(inner[b], fwd_ref[...], preferred_element_type=jnp.float32)
        by_row, by_col = 0.0, 0.0
        for q in range(2):
            rows = pl.ds(row + 8 + q, h, stride=2)
            before, after = pl.ds(row + 7 + q, h, stride=2), pl.ds(row + 9 + q, h, stride=2)
            for k in range(2):
                g_re = wave[q * h : (q + 1) * h, k * lanes : (k + 1) * lanes]
                g_im = wave[q * h : (q + 1) * h, n + k * lanes : n + (k + 1) * lanes]
                p_re, p_im = turned[buf, b, 0, q, k], turned[buf, b, 1, q, k]
                q_re = g_re * p_re + g_im * p_im
                q_im = g_re * p_im - g_im * p_re
                if k == 0:
                    d_re, d_im = (
                        patch[buf, b, part, q, 1 : h + 1, :] - patch[buf, b, part, q, 0:h, :] for part in range(2)
                    )
                    s_re, s_im = (
                        jnp.where(keep, planes[2 + part, block, rows, :], planes[2 + part, block + 2, rows, :])
                        for part in range(2)
                    )
                else:
                    d_re, d_im = (
                        planes[part, block + 1, after, :] - planes[part, block + 1, before, :] for part in range(2)
                    )
                    s_re, s_im = (planes[2 + part, block + 1, rows, :] for part in range(2))
                by_row = by_row + fold(q_re * d_re - q_im * d_im)
                by_col = by_col + fold(q_re * s_re - q_im * s_im)
        for which, value in enumerate((0.5 * by_row, by_col)):
            sums[which, pl.ds(step * batch + b, 1), :] = jnp.sum(value, axis=0, keepdims=True)

    def advance(step, buf):
        later = jnp.minimum(step + 1, steps - 1)
        for b in range(batch):
            along_rows(b)
        for b in range(batch // 2):
            extract(later, b, 1 - buf)
        for b in range(batch):
            residual(step, b)
        for b in range(batch):
            back_rows(b)
        for b in range(batch // 2, batch):
            extract(later, b, 1 - buf)
        for b in range(batch):
            slopes(step, b, buf)

    for b in range(batch):
        extract(0, b, 0)

    @pl.loop(0, steps // 2)
    def _(pair):
        advance(2 * pair, 0)
        advance(2 * pair + 1, 1)

    count = sums.shape[1]
    diagonal = lax.broadcasted_iota(jnp.int32, (count, lanes), 0) == lax.broadcasted_iota(jnp.int32, (count, lanes), 1)
    lines = []
    for which in range(3):
        full = jnp.sum(sums[which], axis=1, keepdims=True)
        lines.append(jnp.sum(jnp.where(diagonal, full, 0.0), axis=0, keepdims=True))
    squares = jnp.sum(lines[0] * lines[0] + lines[1] * lines[1], axis=1, keepdims=True)
    line_ref[...] = jnp.broadcast_to(squares, (1, lanes))
    lines.append(shared_sum(n_tile, n_pos, line_ref, others, sum_sends, sum_recvs))
    out_ref[...] = jnp.concatenate(lines + [jnp.zeros((4, lanes), jnp.float32)], axis=0)


def refine(quarter, probe, frames, offsets, n_tile, n_pos):
    count, n, _ = frames.shape
    _, height, width = quarter.shape
    if count % (2 * BATCH) or count > 128 or n != 2 * 128 or n_pos != 4 or height < n // 2:
        raise ValueError("unsupported sizes")
    forward, backward, pieces = dft_tables(n)
    tall, wide = height * n_pos + n, width + n
    steps = count // BATCH
    devices = n_tile * n_pos
    vmem, dma = pltpu.VMEM, pltpu.SemaphoreType.DMA
    anywhere = pl.BlockSpec(memory_space=pl.ANY)
    return pl.pallas_call(
        functools.partial(refine_kernel, BATCH, steps, n_tile, n_pos),
        out_shape=jax.ShapeDtypeStruct((8, 128), jnp.float32),
        in_specs=[anywhere] * 7,
        out_specs=pl.BlockSpec(memory_space=pltpu.VMEM),
        scratch_shapes=[
            pltpu.SMEM(offsets.shape, jnp.int32),
            vmem((2, tall, wide), jnp.bfloat16),
            vmem((2, 2, n, 128), jnp.float32),
            vmem(forward.shape, jnp.bfloat16),
            vmem(backward.shape, jnp.bfloat16),
            vmem(pieces.shape, jnp.bfloat16),
            vmem(frames.shape, jnp.bfloat16),
            vmem((4, wide // 128, tall + 32, 128), jnp.float32),
            vmem((2, BATCH, 2, 2, n // 2 + 8, 128), jnp.float32),
            vmem((2, BATCH, 2, 2, 2, n // 2, 128), jnp.float32),
            vmem((BATCH, 2, n, n), jnp.bfloat16),
            vmem((BATCH, n, 2 * n), jnp.bfloat16),
            vmem((BATCH, 2, n, n), jnp.bfloat16),
            vmem((BATCH, n, 2 * n), jnp.bfloat16),
            vmem((3, count, 128), jnp.float32),
            dma((SENDS,)),
            dma((RECEIVES,)),
            pltpu.SemaphoreType.REGULAR((GC + n_tile // GC - 2,)),
            dma((10,)),
            vmem((1, 128), jnp.float32),
            vmem((devices - 1, 1, 128), jnp.float32),
            dma((devices - 1,)),
            dma((devices - 1,)),
        ],
        compiler_params=pltpu.CompilerParams(
            vmem_limit_bytes=56 * 1024 * 1024, collective_id=0, has_side_effects=True
        ),
    )(offsets, quarter, probe, frames, forward, backward, pieces)


def scale_kernel(positions, lines_ref, shifts_ref, losses_ref):
    count = shifts_ref.shape[1]
    scale = jnp.sqrt(lines_ref[3:4, :] * (1.0 / positions) + 1e-06)
    shifts_ref[...] = (-lines_ref[0:2, :] / scale)[:, :count]
    losses_ref[...] = lines_ref[2:3, :count]


def normalise(lines, count, positions):
    block = pl.BlockSpec(memory_space=pltpu.VMEM)
    return pl.pallas_call(
        functools.partial(scale_kernel, positions),
        out_shape=(jax.ShapeDtypeStruct((2, count), jnp.float32), jax.ShapeDtypeStruct((1, count), jnp.float32)),
        in_specs=[block],
        out_specs=(block, block),
    )(lines)


def solution(mesh):
    n_tile, n_pos = mesh.shape["tile"], mesh.shape["pos"]

    def local(object_tiles, probe, frames, offsets):
        count = frames.shape[0]
        lines = refine(object_tiles[0], probe, frames, offsets, n_tile, n_pos)
        shifts, losses = normalise(lines, count, count * n_tile * n_pos)
        return shifts, losses[0]

    in_specs = (
        P("tile", None, "pos", None),
        P(),
        P(("tile", "pos"), None, None),
        P(None, ("tile", "pos")),
    )
    out_specs = (P(None, ("tile", "pos")), P(("tile", "pos")))
    return jax.shard_map(local, mesh=mesh, in_specs=in_specs, out_specs=out_specs, check_vma=False)
```

```python
import functools
import math

import jax
import jax.numpy as jnp
import numpy as np
from jax import lax
from jax.experimental import pallas as pl
from jax.experimental.pallas import tpu as pltpu
from jax.sharding import PartitionSpec as P

GC = 4
SENDS = 64
STOPS = 4
RECEIVES = 35
BATCH = 2
MESH_ID = pl.DeviceIdType.MESH


def dft_tables(length_n):
    indices = np.arange(length_n)
    products_mod = indices[:, None] * indices[None, :] % length_n
    angles = products_mod.astype(np.float32) * np.float32(2.0 * math.pi / length_n)
    factor = np.float32(1.0 / math.sqrt(length_n))
    cosine, sine = np.cos(angles) * factor, np.sin(angles) * factor
    forward = np.block([[cosine, sine], [-sine, cosine]])
    low = slice(0, length_n // 2)
    split = [np.block([[cosine[low, q::2], sine[low, q::2]], [-sine[low, q::2], cosine[low, q::2]]]) for q in range(2)]
    pieces = np.stack(split + [piece.T for piece in split])
    return [jnp.asarray(table, jnp.bfloat16) for table in (forward, forward.T, pieces)]


def gather_halo(n_tile, n_pos, margin, x_hbm, pad_ref, send_sems, recv_sems, alive, local_sem, loads, convert):
    t, p = lax.axis_index("tile"), lax.axis_index("pos")
    _, quarter, width = x_hbm.shape
    rows = pad_ref.shape[1] - 2 * margin
    last = rows // quarter - 1
    c, r = t % GC, t // GC
    core, half = p % 2, p // 2
    near, far = p + 1 - 2 * core, p + 2 - 4 * half
    near_far = near + 2 - 4 * half
    west, east = c > 0, c < GC - 1
    north, south = r > 0, r < n_tile // GC - 1
    yes = p >= 0
    both = jnp.logical_and
    tall, wide = rows + 2 * margin, width + 2 * margin

    relatives = [(None, t, (p + k) % n_pos) for k in range(1, n_pos)] + [(west, t - 1, p), (east, t + 1, p)]
    north_far = both(north, jnp.logical_or(p == 0, far == last))
    south_far = both(south, jnp.logical_or(p == last, far == 0))
    relatives += [(north, t - GC, p), (north_far, t - GC, far), (south, t + GC, p), (south_far, t + GC, far)]
    ones = lambda cond: jnp.where(cond, 1, 0)
    count = n_pos - 1 + sum(ones(cond) for cond, _, _ in relatives if cond is not None)

    mine = pl.ds(pl.multiple_of(margin + p * quarter, quarter), quarter)
    own = pltpu.make_async_copy(x_hbm, pad_ref.at[:, mine, margin : margin + width], local_sem)
    own.start()

    def greet(semaphore):
        for cond, to_t, to_p in relatives:
            signal = functools.partial(
                pl.semaphore_signal, semaphore, inc=1, device_id=(to_t, to_p), device_id_type=MESH_ID
            )
            if cond is None:
                signal()
            else:
                pl.when(cond)(signal)

    barrier = pltpu.get_barrier_semaphore()
    greet(barrier)
    for load in loads:
        load.start()
    rounds, share = alive.shape[0], -(-alive.shape[0] // STOPS)

    def spread(stop):
        for k in range(stop * share, min((stop + 1) * share, rounds)):
            pl.semaphore_wait(alive.at[k], count)
            if k + 1 < rounds:
                greet(alive.at[k + 1])

    def block(q):
        return pl.ds(pl.multiple_of(margin + q * quarter, quarter), quarter)

    its, nears, nears_far = block(far), block(near), block(near_far)
    above, below = slice(0, margin), slice(margin + rows, tall)
    top, bottom = slice(margin, 2 * margin), slice(rows, margin + rows)
    mid = slice(margin, margin + width)
    left, right = slice(0, margin), slice(margin + width, wide)
    first_cols, last_cols = slice(margin, 2 * margin), slice(width, margin + width)
    inner_cols = slice(2 * margin, width)
    strips = (first_cols, last_cols, inner_cols)
    sent = []

    def at(rows_at, cols_at):
        return pad_ref.at[:, rows_at, cols_at]

    def zero(cond, rows_at, cols_at):
        @pl.when(cond)
        def _():
            part = at(rows_at, cols_at)
            part[...] = jnp.zeros(part.shape, part.dtype)

    zero(jnp.logical_not(west), slice(0, tall), left)
    zero(jnp.logical_not(east), slice(0, tall), right)
    zero(jnp.logical_not(north), above, slice(0, wide))
    zero(jnp.logical_not(south), below, slice(0, wide))

    def copy(index, src, dst, to_t, to_p, send_index):
        return pltpu.make_async_remote_copy(
            src_ref=src,
            dst_ref=dst,
            send_sem=send_sems.at[send_index],
            recv_sem=recv_sems.at[index],
            device_id=(to_t, to_p),
            device_id_type=MESH_ID,
        )

    def send(cond, index, src, dst, to_t, to_p):
        made = copy(index, src, dst, to_t, to_p, len(sent))
        sent.append((cond, made))

        @pl.when(cond)
        def _():
            made.start()

    def receive(cond, index, dst):
        @pl.when(cond)
        def _():
            copy(index, dst, dst, t, near, 0).wait_recv()

    own.wait()
    pl.semaphore_wait(barrier, count)
    if rounds:
        greet(alive.at[0])

    up, down = both(p == 0, north), both(p == last, south)
    native = jnp.logical_or(up, down)
    buddy = jnp.logical_or(both(near == 0, north), both(near == last, south))
    far_up, far_down = both(far == 0, north), both(far == last, south)
    relays = jnp.logical_or(far_up, far_down)
    plain = jnp.logical_not(jnp.logical_or(native, buddy))
    send(east, 0, at(mine, last_cols), at(mine, left), t + 1, p)
    send(west, 1, at(mine, first_cols), at(mine, right), t - 1, p)
    vertical = ((up, top, below, t - GC, 6), (down, bottom, above, t + GC, 9))
    send(native, 4, at(mine, inner_cols), at(mine, inner_cols), t, far)
    for cond, src, dst, to_t, base in vertical:
        for k in range(2):
            send(cond, base + k, at(src, strips[k]), at(dst, strips[k]), to_t, p)
            send(cond, base + k, at(src, strips[k]), at(dst, strips[k]), to_t, far)
        send(cond, base + 2, at(src, strips[2]), at(dst, strips[2]), to_t, p)
    for k in range(2):
        send(native, 2 + k, at(mine, strips[k]), at(mine, strips[k]), t, far)
    for k in range(3):
        send(plain, 2 + k, at(mine, strips[k]), at(mine, strips[k]), t, far)
    send(yes, 5, at(mine, mid), at(mine, mid), t, near)

    receive(west, 0, at(mine, left))
    receive(east, 1, at(mine, right))
    for k in range(3):
        send(buddy, 2 + k, at(mine, strips[k]), at(mine, strips[k]), t, far)
    send(west, 15, at(mine, left), at(mine, left), t, near)
    send(east, 16, at(mine, right), at(mine, right), t, near)
    spread(0)
    receive(relays, 4, at(its, inner_cols))
    send(far_up, 8, at(top, inner_cols), at(below, inner_cols), t - GC, p)
    send(far_down, 11, at(bottom, inner_cols), at(above, inner_cols), t + GC, p)
    pl.when(jnp.logical_not(north))(lambda: convert(0, margin))
    pl.when(jnp.logical_not(south))(lambda: convert(margin + rows, margin))
    receive(yes, 2, at(its, first_cols))
    send(west, 13, at(its, first_cols), at(its, right), t - 1, p)
    receive(yes, 3, at(its, last_cols))
    send(east, 12, at(its, last_cols), at(its, left), t + 1, p)
    send(yes, 14, at(its, first_cols), at(its, first_cols), t, near)
    send(yes, 33, at(its, last_cols), at(its, last_cols), t, near)
    convert(margin + p * quarter, quarter)
    spread(1)

    halos = ((both(south, core == 0), below, 6, 19, 25), (both(north, core == 1), above, 9, 22, 27))
    for cond, area, base, shared, corner in halos:
        receive(cond, base, at(area, first_cols))
        send(both(cond, west), corner, at(area, first_cols), at(area, right), t - 1, p)
        receive(cond, base + 1, at(area, last_cols))
        send(both(cond, east), corner + 1, at(area, last_cols), at(area, left), t + 1, p)
        send(cond, shared, at(area, first_cols), at(area, first_cols), t, near)
        send(cond, shared + 1, at(area, last_cols), at(area, last_cols), t, near)

    receive(yes, 5, at(nears, mid))
    receive(west, 15, at(nears, left))
    receive(east, 16, at(nears, right))
    convert(margin + near * quarter, quarter)
    spread(2)

    for cond, area, base, shared, corner in halos:
        receive(cond, base + 2, at(area, inner_cols))
        send(cond, shared + 2, at(area, inner_cols), at(area, inner_cols), t, near)
    receive(jnp.logical_not(relays), 4, at(its, inner_cols))
    send(yes, 34, at(its, inner_cols), at(its, inner_cols), t, near)
    receive(east, 13, at(its, right))
    send(east, 18, at(its, right), at(its, right), t, near)
    receive(west, 12, at(its, left))
    send(west, 17, at(its, left), at(its, left), t, near)
    for cond, area, base, shared, corner in halos:
        receive(both(cond, east), corner, at(area, right))
        send(both(cond, east), corner + 4, at(area, right), at(area, right), t, near)
        receive(both(cond, west), corner + 1, at(area, left))
        send(both(cond, west), corner + 5, at(area, left), at(area, left), t, near)
    convert(margin + far * quarter, quarter)
    spread(3)

    receive(yes, 14, at(nears_far, first_cols))
    receive(yes, 33, at(nears_far, last_cols))
    receive(west, 17, at(nears_far, left))
    receive(east, 18, at(nears_far, right))
    receive(yes, 34, at(nears_far, inner_cols))
    convert(margin + near_far * quarter, quarter)
    others = ((both(south, core == 1), below, 19, 25), (both(north, core == 0), above, 22, 27))
    for cond, area, shared, corner in others:
        for k in range(3):
            receive(cond, shared + k, at(area, strips[k]))
        receive(both(cond, east), corner + 4, at(area, right))
        receive(both(cond, west), corner + 5, at(area, left))
    pl.when(north)(lambda: convert(0, margin))
    pl.when(south)(lambda: convert(margin + rows, margin))
    for cond, made in sent:
        @pl.when(cond)
        def _():
            made.wait_send()


def shared_sum(n_tile, n_pos, mine_ref, others, send_sems, recv_sems):
    me = lax.axis_index("tile") * n_pos + lax.axis_index("pos")
    count = n_tile * n_pos
    copies = []
    for k in range(1, count):
        other = lax.rem(me + k, count)
        made = pltpu.make_async_remote_copy(
            src_ref=mine_ref,
            dst_ref=others.at[k - 1],
            send_sem=send_sems.at[k - 1],
            recv_sem=recv_sems.at[k - 1],
            device_id=(other // n_pos, other % n_pos),
            device_id_type=MESH_ID,
        )
        made.start()
        copies.append(made)
    for made in copies:
        made.wait()
    return jnp.sum(others[...], axis=0) + mine_ref[...]


def fold(value):
    return jnp.sum(value.reshape(-1, 8, value.shape[-1]), axis=0)


def refine_kernel(
    batch, steps, n_tile, n_pos, off_hbm, x_hbm, probe_hbm, frames_hbm, fwd_hbm, bwd_hbm, pieces_hbm, out_ref,
    off_ref, pad_ref, probe_ref, fwd_ref, bwd_ref, pieces_ref, frames_ref, planes, patch, turned, exits, halves, resid, inner,
    sums, send_sems, recv_sems, alive, local_sems, line_ref, others, sum_sends, sum_recvs,
):
    n = probe_ref.shape[2]
    h = n // 2
    tall, wide = pad_ref.shape[1], pad_ref.shape[2]
    lanes = 128

    def convert(first, height):
        @pl.loop(0, height // 32)
        def _(i):
            at = pl.ds(pl.multiple_of(first + i * 32, 32), 32)
            lower = pl.ds(pl.multiple_of(first + i * 32 + 8, 8), 32)
            for part in range(2):
                value = pad_ref[part, at, :].astype(jnp.float32)
                slope = 0.5 * (pltpu.roll(value, wide - 1, 1) - pltpu.roll(value, 1, 1))
                for k in range(wide // lanes):
                    cols = slice(k * lanes, (k + 1) * lanes)
                    planes[part, k, lower, :] = value[:, cols]
                    planes[2 + part, k, lower, :] = slope[:, cols]

    pairs = [(off_hbm, off_ref), (fwd_hbm, fwd_ref), (bwd_hbm, bwd_ref), (pieces_hbm, pieces_ref), (frames_hbm, frames_ref)]
    for part in range(2):
        for k in range(2):
            pairs.append((probe_hbm.at[part, :, pl.ds(k * lanes, lanes)], probe_ref.at[part, k]))
    loads = [pltpu.make_async_copy(source, target, local_sems.at[k + 1]) for k, (source, target) in enumerate(pairs)]
    gather_halo(n_tile, n_pos, n // 2, x_hbm, pad_ref, send_sems, recv_sems, alive, local_sems.at[0], loads, convert)
    for load in loads:
        load.wait()

    lane = lax.broadcasted_iota(jnp.int32, (1, lanes), 1)

    def place(step, b):
        j = step * batch + b
        row, col = off_ref[0, j], off_ref[1, j]
        return row, col // lanes, col % lanes

    def extract(step, b, buf):
        row, block, shift = place(step, b)
        keep = lane >= shift
        for part in range(2):
            for seq in range(2):
                rows = pl.ds(row + 7 + seq, h + 8, stride=2)
                patch[buf, b, part, seq] = jnp.where(keep, planes[part, block, rows, :], planes[part, block + 2, rows, :])
        for q in range(2):
            rows = pl.ds(row + 8 + q, h, stride=2)
            for part in range(2):
                ends = [pltpu.roll(probe_ref[part, k, pl.ds(q, h, stride=2), :], shift, 1) for k in range(2)]
                turned[buf, b, part, q, 0] = jnp.where(keep, ends[0], ends[1])
                turned[buf, b, part, q, 1] = jnp.where(keep, ends[1], ends[0])
            for k in range(2):
                cols = slice(k * lanes, (k + 1) * lanes)
                if k == 0:
                    o_re, o_im = (patch[buf, b, part, 1 - q, q : q + h, :] for part in range(2))
                else:
                    o_re, o_im = (planes[part, block + 1, rows, :] for part in range(2))
                p_re, p_im = turned[buf, b, 0, q, k], turned[buf, b, 1, q, k]
                exits[b, q, :h, cols] = (p_re * o_re - p_im * o_im).astype(jnp.bfloat16)
                exits[b, q, h:, cols] = (p_re * o_im + p_im * o_re).astype(jnp.bfloat16)

    def along_rows(b):
        evens = jnp.dot(pieces_ref[0], exits[b, 0], preferred_element_type=jnp.float32)
        odds = jnp.dot(pieces_ref[1], exits[b, 1], preferred_element_type=jnp.float32)
        plus, minus = (evens + odds).astype(jnp.bfloat16), (evens - odds).astype(jnp.bfloat16)
        halves[b, :h, :n], halves[b, :h, n:] = plus[:h], plus[h:]
        halves[b, h:, :n], halves[b, h:, n:] = minus[:h], minus[h:]

    def residual(step, b):
        wave = jnp.dot(halves[b], bwd_ref[...], preferred_element_type=jnp.float32)
        f_re, f_im = wave[:, :n], wave[:, n:]
        square = f_re * f_re + f_im * f_im
        frame = frames_ref[step * batch + b].astype(jnp.float32)
        keep_part = 1.0 - frame * lax.rsqrt(jnp.maximum(square, 0.0625))
        r_re, r_im = f_re * keep_part, f_im * keep_part
        resid[b, 0, :h, :] = (r_re[:h] + r_re[h:]).astype(jnp.bfloat16)
        resid[b, 0, h:, :] = (r_im[:h] + r_im[h:]).astype(jnp.bfloat16)
        resid[b, 1, :h, :] = (r_re[:h] - r_re[h:]).astype(jnp.bfloat16)
        resid[b, 1, h:, :] = (r_im[:h] - r_im[h:]).astype(jnp.bfloat16)
        loss = fold(square * (keep_part * keep_part)) * (1.0 / (n * n))
        sums[2, pl.ds(step * batch + b, 1), :] = jnp.sum(loss[:, :lanes] + loss[:, lanes:], axis=0, keepdims=True)

    def back_rows(b):
        for q in range(2):
            back = jnp.dot(pieces_ref[2 + q], resid[b, q], preferred_element_type=jnp.float32).astype(jnp.bfloat16)
            inner[b, q * h : (q + 1) * h, :n] = back[:h]
            inner[b, q * h : (q + 1) * h, n:] = back[h:]

    def slopes(step, b, buf):
        row, block, shift = place(step, b)
        keep = lane >= shift
        wave = jnp.dot(inner[b], fwd_ref[...], preferred_element_type=jnp.float32)
        by_row, by_col = 0.0, 0.0
        for q in range(2):
            rows = pl.ds(row + 8 + q, h, stride=2)
            before, after = pl.ds(row + 7 + q, h, stride=2), pl.ds(row + 9 + q, h, stride=2)
            for k in range(2):
                g_re = wave[q * h : (q + 1) * h, k * lanes : (k + 1) * lanes]
                g_im = wave[q * h : (q + 1) * h, n + k * lanes : n + (k + 1) * lanes]
                p_re, p_im = turned[buf, b, 0, q, k], turned[buf, b, 1, q, k]
                q_re = g_re * p_re + g_im * p_im
                q_im = g_re * p_im - g_im * p_re
                if k == 0:
                    d_re, d_im = (
                        patch[buf, b, part, q, 1 : h + 1, :] - patch[buf, b, part, q, 0:h, :] for part in range(2)
                    )
                    s_re, s_im = (
                        jnp.where(keep, planes[2 + part, block, rows, :], planes[2 + part, block + 2, rows, :])
                        for part in range(2)
                    )
                else:
                    d_re, d_im = (
                        planes[part, block + 1, after, :] - planes[part, block + 1, before, :] for part in range(2)
                    )
                    s_re, s_im = (planes[2 + part, block + 1, rows, :] for part in range(2))
                by_row = by_row + fold(q_re * d_re - q_im * d_im)
                by_col = by_col + fold(q_re * s_re - q_im * s_im)
        for which, value in enumerate((0.5 * by_row, by_col)):
            sums[which, pl.ds(step * batch + b, 1), :] = jnp.sum(value, axis=0, keepdims=True)

    def advance(step, buf):
        later = jnp.minimum(step + 1, steps - 1)
        for b in range(batch):
            along_rows(b)
        for b in range(batch):
            residual(step, b)
        for b in range(batch):
            back_rows(b)
        for b in range(batch):
            slopes(step, b, buf)
        for b in range(batch):
            extract(later, b, 1 - buf)

    for b in range(batch):
        extract(0, b, 0)

    @pl.loop(0, steps // 2)
    def _(pair):
        advance(2 * pair, 0)
        advance(2 * pair + 1, 1)

    count = sums.shape[1]
    diagonal = lax.broadcasted_iota(jnp.int32, (count, lanes), 0) == lax.broadcasted_iota(jnp.int32, (count, lanes), 1)
    lines = []
    for which in range(3):
        full = jnp.sum(sums[which], axis=1, keepdims=True)
        lines.append(jnp.sum(jnp.where(diagonal, full, 0.0), axis=0, keepdims=True))
    squares = jnp.sum(lines[0] * lines[0] + lines[1] * lines[1], axis=1, keepdims=True)
    line_ref[...] = jnp.broadcast_to(squares, (1, lanes))
    lines.append(shared_sum(n_tile, n_pos, line_ref, others, sum_sends, sum_recvs))
    out_ref[...] = jnp.concatenate(lines + [jnp.zeros((4, lanes), jnp.float32)], axis=0)


def refine(quarter, probe, frames, offsets, n_tile, n_pos):
    count, n, _ = frames.shape
    _, height, width = quarter.shape
    if count % (2 * BATCH) or count > 128 or n != 2 * 128 or n_pos != 4 or height < n // 2:
        raise ValueError("unsupported sizes")
    forward, backward, pieces = dft_tables(n)
    tall, wide = height * n_pos + n, width + n
    steps = count // BATCH
    devices = n_tile * n_pos
    vmem, dma = pltpu.VMEM, pltpu.SemaphoreType.DMA
    anywhere = pl.BlockSpec(memory_space=pl.ANY)
    return pl.pallas_call(
        functools.partial(refine_kernel, BATCH, steps, n_tile, n_pos),
        out_shape=jax.ShapeDtypeStruct((8, 128), jnp.float32),
        in_specs=[anywhere] * 7,
        out_specs=pl.BlockSpec(memory_space=pltpu.VMEM),
        scratch_shapes=[
            pltpu.SMEM(offsets.shape, jnp.int32),
            vmem((2, tall, wide), jnp.bfloat16),
            vmem((2, 2, n, 128), jnp.float32),
            vmem(forward.shape, jnp.bfloat16),
            vmem(backward.shape, jnp.bfloat16),
            vmem(pieces.shape, jnp.bfloat16),
            vmem(frames.shape, jnp.bfloat16),
            vmem((4, wide // 128, tall + 32, 128), jnp.float32),
            vmem((2, BATCH, 2, 2, n // 2 + 8, 128), jnp.float32),
            vmem((2, BATCH, 2, 2, 2, n // 2, 128), jnp.float32),
            vmem((BATCH, 2, n, n), jnp.bfloat16),
            vmem((BATCH, n, 2 * n), jnp.bfloat16),
            vmem((BATCH, 2, n, n), jnp.bfloat16),
            vmem((BATCH, n, 2 * n), jnp.bfloat16),
            vmem((3, count, 128), jnp.float32),
            dma((SENDS,)),
            dma((RECEIVES,)),
            pltpu.SemaphoreType.REGULAR((GC + n_tile // GC - 2,)),
            dma((10,)),
            vmem((1, 128), jnp.float32),
            vmem((devices - 1, 1, 128), jnp.float32),
            dma((devices - 1,)),
            dma((devices - 1,)),
        ],
        compiler_params=pltpu.CompilerParams(
            vmem_limit_bytes=56 * 1024 * 1024, collective_id=0, has_side_effects=True
        ),
    )(offsets, quarter, probe, frames, forward, backward, pieces)


def scale_kernel(positions, lines_ref, shifts_ref, losses_ref):
    count = shifts_ref.shape[1]
    scale = jnp.sqrt(lines_ref[3:4, :] * (1.0 / positions) + 1e-06)
    shifts_ref[...] = (-lines_ref[0:2, :] / scale)[:, :count]
    losses_ref[...] = lines_ref[2:3, :count]


def normalise(lines, count, positions):
    block = pl.BlockSpec(memory_space=pltpu.VMEM)
    return pl.pallas_call(
        functools.partial(scale_kernel, positions),
        out_shape=(jax.ShapeDtypeStruct((2, count), jnp.float32), jax.ShapeDtypeStruct((1, count), jnp.float32)),
        in_specs=[block],
        out_specs=(block, block),
    )(lines)


def solution(mesh):
    n_tile, n_pos = mesh.shape["tile"], mesh.shape["pos"]

    def local(object_tiles, probe, frames, offsets):
        count = frames.shape[0]
        lines = refine(object_tiles[0], probe, frames, offsets, n_tile, n_pos)
        shifts, losses = normalise(lines, count, count * n_tile * n_pos)
        return shifts, losses[0]

    in_specs = (
        P("tile", None, "pos", None),
        P(),
        P(("tile", "pos"), None, None),
        P(None, ("tile", "pos")),
    )
    out_specs = (P(None, ("tile", "pos")), P(("tile", "pos")))
    return jax.shard_map(local, mesh=mesh, in_specs=in_specs, out_specs=out_specs, check_vma=False)
```
